512 devices in a mesh: cable: 256 (over z, y, x), win: 2 (over core).
Axes of the slice: x: 4, y: 8, z: 8, core: 2. Of those that a mesh axis runs over, the one named last changes fastest.
Arguments:
- records: bfloat16 [512, 8192, 128], P(None, 'cable', 'win'), may hold values from -60 to 60
Outputs:
- xcorr: float32 [8192, 64, 512], P('cable', None, 'win')
The draws below stay inside these ranges and needn't reach their ends.
All inputs are finite; a program needn't handle non-finite values.
Results may differ from the reference program's by a relative error of at most 0.0064.
Values may be sent and summed in bfloat16 or wider, within the bound.
A program may use at most 128 MiB of HBM per device.

```python
import math
import jax
import jax.numpy as jnp
from jax import lax

SAMPLES = 512
OFFS = 64
CHANNELS = 8192
WINDOWS = 128


def draw_records(key, part):
    keys = jax.random.split(jax.random.fold_in(key, 17), 3)
    base = jax.random.normal(keys[0], (SAMPLES, CHANNELS, WINDOWS), jnp.float32)
    colour = jax.random.uniform(keys[1], (1, CHANNELS, 1), jnp.float32, -0.8, 0.8)
    mixed = base + colour * jnp.roll(base, 1, axis=0)
    scale = jnp.exp(jax.random.uniform(keys[2], (1, CHANNELS, WINDOWS), jnp.float32, 0.0, math.log(10.0)))
    return jnp.clip(mixed * scale, -60.0, 60.0).astype(jnp.bfloat16)


def setup_inputs(seed: int = 0) -> dict:
    streams_of = jax.random.split(jax.random.key(seed), 2)
    records = draw_records(jax.random.fold_in(streams_of[1], 71), 0)
    return {"records": records}


epsilon = 1e-06

def forward_table(samples):
    frequencies = samples // 2 + 1
    times = jnp.arange(samples, dtype=jnp.int32)[None, :]
    freq = jnp.arange(frequencies, dtype=jnp.int32)[:, None]
    phase = 2.0 * math.pi / samples * (freq * times % samples).astype(jnp.float32)
    taper = 0.5 - 0.5 * jnp.cos(2.0 * math.pi / samples * times.astype(jnp.float32))
    return jnp.concatenate([taper * jnp.cos(phase), -taper * jnp.sin(phase)], axis=0).astype(jnp.bfloat16)

def inverse_table(samples, lag_start, lag_count, factor):
    frequencies = samples // 2 + 1
    freq = jnp.arange(frequencies, dtype=jnp.int32)[:, None]
    lagpos = lag_start + jnp.arange(lag_count, dtype=jnp.int32)[None, :]
    phase = 2.0 * math.pi / samples * (freq * lagpos % samples).astype(jnp.float32)
    weight = jnp.where((freq == 0) | (freq == samples // 2), 1.0, 2.0).astype(jnp.float32) * factor
    return jnp.concatenate([weight * jnp.cos(phase), -weight * jnp.sin(phase)], axis=0)

def reference(records):
    samples, channels, windows = records.shape
    frequencies = samples // 2 + 1
    table = forward_table(samples)
    spectra = jnp.dot(table, records.reshape(samples, channels * windows), preferred_element_type=jnp.float32)
    spectra = spectra.reshape(2 * frequencies, channels, windows)
    real_part = spectra[:frequencies]
    imag_part = spectra[frequencies:]
    power = lax.optimization_barrier(jnp.sum(real_part * real_part + imag_part * imag_part, axis=2)) / windows
    scaling = lax.rsqrt(power + epsilon)[:, :, None]
    packed = jnp.concatenate([real_part * scaling, imag_part * scaling], axis=2).astype(jnp.bfloat16)
    flipped = jnp.concatenate([packed[:, :, windows:], -packed[:, :, :windows]], axis=2)
    padded = jnp.pad(packed, ((0, 0), (0, OFFS), (0, 0)))
    lefthand = packed.astype(jnp.float32)
    flipped_wide = flipped.astype(jnp.float32)

    def one_offset(offset):
        partner = lax.dynamic_slice_in_dim(padded, (offset + 1).astype(jnp.int32), channels, 1).astype(jnp.float32)
        real_sum = lax.optimization_barrier(jnp.sum(lefthand * partner, axis=2))
        imag_sum = lax.optimization_barrier(jnp.sum(flipped_wide * partner, axis=2))
        return jnp.concatenate([real_sum, imag_sum], axis=0)
    cross = lax.map(one_offset, jnp.arange(OFFS, dtype=jnp.int32))
    factor = 1.0 / math.sqrt(2.0 * windows * frequencies)
    inverse = inverse_table(samples, 0, samples, factor)
    return jnp.einsum('kxc,xl->ckl', cross, inverse, precision=lax.Precision.HIGHEST)
```

```python
import functools
import math

import jax
import jax.numpy as jnp
import numpy as np
from jax import lax
from jax.experimental import pallas as pl
from jax.experimental.pallas import tpu as pltpu
from jax.sharding import PartitionSpec as P

MESH = pl.DeviceIdType.MESH

OFFS = 64
SAMPLES = 512
CH = 32
ROW = 4
SLOTS = 33
FREQS = ROW * SLOTS
PADDED = 136
LAGS = 256

epsilon = 1e-06


def slot_frequencies(parity):
    place = np.arange(PADDED)
    chip, slot = place // SLOTS, place % SLOTS
    half = np.where(slot < 32, 32 * chip + slot, 128)
    held = np.where(slot < 32, chip < ROW, (chip == ROW - 1) & (parity == 0))
    return (2 * half + parity)[:, None], held[:, None]


def angles(freq, times):
    return np.float32(2.0 * math.pi / SAMPLES) * (freq * times % SAMPLES).astype(np.float32)


def forward_table(parity):
    freq, held = slot_frequencies(parity)
    times = np.arange(SAMPLES)[None, :]
    phase = angles(freq, times)
    taper = np.float32(0.5) - np.float32(0.5) * np.cos(angles(1, times))
    taper = np.where(held, taper, np.float32(0.0))
    both = np.concatenate([taper * np.cos(phase), -taper * np.sin(phase)], axis=0)
    return both.astype(jnp.bfloat16)


def inverse_table(parity, factor):
    freq, held = slot_frequencies(parity)
    freq, held = freq[:FREQS], held[:FREQS]
    phase = angles(freq, np.arange(LAGS)[None, :])
    weight = np.where((freq == 0) | (freq == SAMPLES // 2), 1.0, 2.0) * held * factor
    weight = weight.astype(np.float32)
    both = np.stack([weight * np.cos(phase), -weight * np.sin(phase)], axis=1)
    return both.reshape(2 * FREQS, LAGS).astype(jnp.bfloat16)


def whiten_kernel(windows, table_ref, own_ref, other_ref, white_ref, re_buf, im_buf):
    core = lax.axis_index("win")

    @pl.loop(0, CH // 2, unroll=2)
    def _(pair):
        c = 2 * pair
        rhs = jnp.concatenate(
            [own_ref[c], other_ref[c], own_ref[c + 1], other_ref[c + 1]], axis=0
        )
        spectra = lax.dot_general(
            table_ref[core], rhs, (((1,), (1,)), ((), ())), preferred_element_type=jnp.float32
        )
        for half in range(2):
            re = spectra[:PADDED, 128 * half : 128 * half + 128]
            im = spectra[PADDED:, 128 * half : 128 * half + 128]
            power = jnp.sum(re * re + im * im, axis=1, keepdims=True)
            scaling = lax.rsqrt(power / windows + epsilon)
            re_buf[pl.ds(c + half, PADDED, stride=CH), :] = re * scaling
            im_buf[pl.ds(c + half, PADDED, stride=CH), :] = im * scaling

    @pl.loop(0, FREQS, unroll=4)
    def _(f):
        rows = pl.ds(pl.multiple_of(f * CH, CH), CH)
        white_ref[f, :, 0:128] = re_buf[rows, :].astype(jnp.bfloat16)
        white_ref[f, :, 128:256] = im_buf[rows, :].astype(jnp.bfloat16)


def spread_kernel(rows, white_ref, group_ref, halo_ref, send, recv, halo_send, halo_recv, local):
    me = lax.axis_index("cable")
    core = lax.axis_index("win")
    x, row = lax.rem(me, ROW), lax.div(me, ROW)
    base = row * ROW
    before = lax.rem(row + rows - 1, rows) * ROW + x
    after = lax.rem(row + 1, rows) * ROW + x
    peers = [base + lax.rem(x + d, ROW) for d in range(1, ROW)]
    barrier = pltpu.get_barrier_semaphore()
    for peer in [*peers, before, after]:
        pl.semaphore_signal(barrier, inc=1, device_id=(peer, core), device_id_type=MESH)
    pl.semaphore_wait(barrier, 5)

    own = pltpu.make_async_copy(white_ref.at[x], group_ref.at[x], local)
    own.start()
    copies = []
    for d in (1, 3, 2):
        copy = pltpu.make_async_remote_copy(
            src_ref=white_ref.at[lax.rem(x + d, ROW)],
            dst_ref=group_ref.at[x],
            send_sem=send.at[d],
            recv_sem=recv.at[d],
            device_id=(peers[d - 1], core),
            device_id_type=MESH,
        )
        copy.start()
        copies.append(copy)
    own.wait()
    for copy in copies:
        copy.wait()
    halos = []
    for b in range(2):
        copy = pltpu.make_async_remote_copy(
            src_ref=group_ref.at[b],
            dst_ref=halo_ref.at[b],
            send_sem=halo_send.at[b],
            recv_sem=halo_recv.at[b],
            device_id=(before, core),
            device_id_type=MESH,
        )
        copy.start()
        halos.append(copy)
    for copy in halos:
        copy.wait()


def skewed(product):
    lane = lax.broadcasted_iota(jnp.int32, (8, 128), 1)
    back = 7 - lax.broadcasted_iota(jnp.int32, (8, 128), 0)
    turned = []
    for v in range(4):
        group = jnp.take_along_axis(product[8 * v : 8 * v + 8], back, axis=0)
        shift = (120 - 8 * v + 64 * (v // 2)) % 128
        turned.append(pltpu.roll(group, shift, 1, stride=1, stride_axis=0))
    both = [jnp.where(lane < OFFS, turned[v], turned[v + 2]) for v in range(2)]
    return jnp.concatenate(both, axis=0).astype(jnp.bfloat16)


def cross_kernel(rows, group_ref, halo_ref, cross_ref):
    last = lax.div(lax.axis_index("cable"), ROW) == rows - 1

    @pl.loop(0, SLOTS, unroll=3)
    def _(f):
        blocks = [group_ref[b, f] for b in range(ROW)]
        for b in range(2):
            halo = halo_ref[b, f]
            blocks.append(jnp.where(last, jnp.zeros_like(halo), halo))
        for b in range(ROW):
            mine = blocks[b]
            flipped = jnp.concatenate([mine[:, 128:], -mine[:, :128]], axis=1)
            lhs = jnp.concatenate([mine, flipped], axis=0)
            rhs = jnp.concatenate([*blocks[b : b + 3], mine], axis=0)
            product = lax.dot_general(
                lhs, rhs, (((1,), (1,)), ((), ())), preferred_element_type=jnp.float32
            )
            for part in range(2):
                cross_ref[b, 2 * f + part] = skewed(product[32 * part : 32 * part + 32])


def gather_kernel(cross_ref, out_ref, send, recv, local):
    me = lax.axis_index("cable")
    core = lax.axis_index("win")
    x, row = lax.rem(me, ROW), lax.div(me, ROW)
    base = row * ROW
    peers = [base + lax.rem(x + d, ROW) for d in range(1, ROW)]
    barrier = pltpu.get_barrier_semaphore()
    for peer in peers:
        pl.semaphore_signal(barrier, inc=1, device_id=(peer, core), device_id_type=MESH)
    pl.semaphore_wait(barrier, 3)
    own = pltpu.make_async_copy(cross_ref.at[x], out_ref.at[x], local)
    own.start()
    copies = []
    for d in (1, 3, 2):
        copy = pltpu.make_async_remote_copy(
            src_ref=cross_ref.at[lax.rem(x + d, ROW)],
            dst_ref=out_ref.at[x],
            send_sem=send.at[d],
            recv_sem=recv.at[d],
            device_id=(peers[d - 1], core),
            device_id_type=MESH,
        )
        copy.start()
        copies.append(copy)
    own.wait()
    for copy in copies:
        copy.wait()


def back_kernel(cross_ref, inverse_ref, out_ref, buf):
    core = lax.axis_index("win")
    terms = 2 * FREQS

    @pl.loop(0, terms, unroll=8)
    def _(g):
        buf[pl.ds(g, 16, stride=terms), :] = cross_ref[g].astype(jnp.float32)

    @pl.loop(0, 16, unroll=2)
    def _(p):
        c = 8 * (p // 8) + 7 - p % 8
        spectrum = buf[pl.ds(pl.multiple_of(p * terms, 8), terms), :].astype(jnp.bfloat16)
        lags = lax.dot_general(
            spectrum,
            inverse_ref[core],
            (((0,), (0,)), ((), ())),
            preferred_element_type=jnp.float32,
        )
        out_ref[c] = lags[:OFFS]
        out_ref[c + 16] = lags[OFFS:]


VMEM = pl.BlockSpec(memory_space=pltpu.VMEM)
ANY = pl.BlockSpec(memory_space=pl.ANY)


def body(rows, records):
    samples, channels, windows = records.shape
    assert (samples, channels) == (SAMPLES, CH)
    total_windows = 2 * windows
    core = lax.axis_index("win")
    own = jnp.transpose(records, (1, 2, 0))
    other = lax.ppermute(own, "win", [(0, 1), (1, 0)])
    tables = np.stack([forward_table(0), forward_table(1)])
    factor = 1.0 / math.sqrt(2.0 * total_windows * (samples // 2 + 1))
    inverses = np.stack([inverse_table(0, factor), inverse_table(1, factor)])
    bf16 = jnp.bfloat16
    white = pl.pallas_call(
        functools.partial(whiten_kernel, total_windows),
        out_shape=jax.ShapeDtypeStruct((FREQS, CH, 256), bf16),
        in_specs=[VMEM] * 3,
        out_specs=VMEM,
        scratch_shapes=[pltpu.VMEM((PADDED * CH, 128), jnp.float32)] * 2,
        name="whiten",
    )(tables, own, other)
    white = white.reshape(ROW, SLOTS, CH, 256)
    group, halo = pl.pallas_call(
        functools.partial(spread_kernel, rows),
        out_shape=[
            jax.ShapeDtypeStruct((ROW, SLOTS, CH, 256), bf16),
            jax.ShapeDtypeStruct((2, SLOTS, CH, 256), bf16),
        ],
        in_specs=[ANY],
        out_specs=[ANY, ANY],
        scratch_shapes=[
            pltpu.SemaphoreType.DMA((4,)),
            pltpu.SemaphoreType.DMA((4,)),
            pltpu.SemaphoreType.DMA((2,)),
            pltpu.SemaphoreType.DMA((2,)),
            pltpu.SemaphoreType.DMA,
        ],
        compiler_params=pltpu.CompilerParams(collective_id=0, has_side_effects=True),
        name="spread",
    )(white)
    cross = pl.pallas_call(
        functools.partial(cross_kernel, rows),
        out_shape=jax.ShapeDtypeStruct((ROW, 2 * SLOTS, 16, 128), bf16),
        in_specs=[VMEM] * 2,
        out_specs=VMEM,
        name="cross",
    )(group, halo)
    spectrum = pl.pallas_call(
        gather_kernel,
        out_shape=jax.ShapeDtypeStruct((ROW, 2 * SLOTS, 16, 128), bf16),
        in_specs=[ANY],
        out_specs=ANY,
        scratch_shapes=[
            pltpu.SemaphoreType.DMA((4,)),
            pltpu.SemaphoreType.DMA((4,)),
            pltpu.SemaphoreType.DMA,
        ],
        compiler_params=pltpu.CompilerParams(collective_id=1, has_side_effects=True),
        name="gather",
    )(cross)
    spectrum = spectrum.reshape(2 * FREQS, 16, 128)
    half = pl.pallas_call(
        back_kernel,
        out_shape=jax.ShapeDtypeStruct((CH, OFFS, LAGS), jnp.float32),
        in_specs=[VMEM] * 2,
        out_specs=VMEM,
        scratch_shapes=[pltpu.VMEM((16 * 2 * FREQS, 128), jnp.float32)],
        name="back",
    )(spectrum, inverses)
    theirs = lax.ppermute(half.astype(bf16), "win", [(0, 1), (1, 0)]).astype(jnp.float32)
    return jnp.where(core == 0, half, -half) + theirs


def solution(mesh):
    rows = mesh.shape["cable"] // ROW
    return jax.shard_map(
        functools.partial(body, rows),
        mesh=mesh,
        in_specs=(P(None, "cable", "win"),),
        out_specs=P("cable", None, "win"),
        check_vma=False,
    )
```

```python
import functools
import math

import jax
import jax.numpy as jnp
import numpy as np
from jax import lax
from jax.experimental import pallas as pl
from jax.experimental.pallas import tpu as pltpu
from jax.sharding import PartitionSpec as P

MESH = pl.DeviceIdType.MESH

OFFS = 64
SAMPLES = 512
CH = 32
ROW = 4
CHUNKS = 3
PART = 11
FREQS = ROW * PART
PADDED = 48
TERMS = 2 * FREQS
LAGS = 256
PIECES = 4

epsilon = 1e-06


def chunk_frequencies(parity, chunk):
    place = np.arange(PADDED)
    chip, slot = place // PART, chunk * PART + place % PART
    half = np.where(slot < 32, 32 * chip + slot, 128)
    held = np.where(slot < 32, chip < ROW, (chip == ROW - 1) & (parity == 0))
    return (2 * half + parity)[:, None], held[:, None]


def angles(freq, times):
    return np.float32(2.0 * math.pi / SAMPLES) * (freq * times % SAMPLES).astype(np.float32)


def forward_table(parity, chunk):
    freq, held = chunk_frequencies(parity, chunk)
    times = np.arange(SAMPLES)[None, :]
    phase = angles(freq, times)
    taper = np.float32(0.5) - np.float32(0.5) * np.cos(angles(1, times))
    taper = np.where(held, taper, np.float32(0.0))
    both = np.concatenate([taper * np.cos(phase), -taper * np.sin(phase)], axis=0)
    return both.astype(jnp.bfloat16)


def inverse_table(parity, chunk, factor):
    freq, held = chunk_frequencies(parity, chunk)
    freq, held = freq[:FREQS], held[:FREQS]
    phase = angles(freq, np.arange(LAGS)[None, :])
    weight = np.where((freq == 0) | (freq == SAMPLES // 2), 1.0, 2.0) * held * factor
    weight = weight.astype(np.float32)
    both = np.stack([weight * np.cos(phase), -weight * np.sin(phase)], axis=1)
    return both.reshape(TERMS, LAGS).astype(jnp.bfloat16)


def skewed(product):
    lane = lax.broadcasted_iota(jnp.int32, (8, 128), 1)
    back = 7 - lax.broadcasted_iota(jnp.int32, (8, 128), 0)
    turned = []
    for v in range(4):
        group = jnp.take_along_axis(product[8 * v : 8 * v + 8], back, axis=0)
        shift = (120 - 8 * v + 64 * (v // 2)) % 128
        turned.append(pltpu.roll(group, shift, 1, stride=1, stride_axis=0))
    both = [jnp.where(lane < OFFS, turned[v], turned[v + 2]) for v in range(2)]
    return jnp.concatenate(both, axis=0).astype(jnp.bfloat16)


def kernel(
    rows,
    windows,
    table_ref,
    inverse_ref,
    own_ref,
    out_ref,
    other,
    re_buf,
    im_buf,
    white,
    group,
    relayed,
    halo,
    cross,
    cross_relayed,
    back,
    turned,
    mine_out,
    theirs_in,
    pair_send,
    pair_recv,
    white_send,
    white_recv,
    relay_recv,
    forward_send,
    halo_send,
    halo_recv,
    cross_send,
    cross_recv,
    cross_relay_recv,
    cross_forward_send,
    out_send,
    out_recv,
):
    me = lax.axis_index("cable")
    core = lax.axis_index("win")
    x, row = lax.rem(me, ROW), lax.div(me, ROW)
    base = row * ROW

    def chip(distance):
        return lax.rem(x + distance, ROW)

    around = 1 + 2 * core
    opposite = 4 - around
    before = lax.rem(row + rows - 1, rows) * ROW + x
    after = lax.rem(row + 1, rows) * ROW + x
    partner = (me, 1 - core)
    barrier = pltpu.get_barrier_semaphore()
    for device in [
        partner,
        (base + chip(1), core),
        (base + chip(3), core),
        (before, core),
        (after, core),
    ]:
        pl.semaphore_signal(barrier, inc=1, device_id=device, device_id_type=MESH)
    pl.semaphore_wait(barrier, 5)

    sent = []

    def send(source, target, send_sem, recv_sem, device):
        copy = pltpu.make_async_remote_copy(
            src_ref=source,
            dst_ref=target,
            send_sem=send_sem,
            recv_sem=recv_sem,
            device_id=device,
            device_id_type=MESH,
        )
        copy.start()
        sent.append(copy)
        return copy

    def arrived(target, sem):
        pltpu.make_async_copy(target, target, sem).wait()

    def spread(source, target, relay, sends, recvs, relay_sem):
        relay_to = (base + chip(around), core)
        send(source.at[chip(2)], relay, sends.at[2], relay_sem, relay_to)
        for distance in (1, 3):
            send(
                source.at[chip(distance)],
                target.at[x],
                sends.at[distance],
                recvs.at[4 - distance],
                (base + chip(distance), core),
            )
        pltpu.make_async_copy(source.at[x], target.at[x], recvs.at[0]).start()

    def forward(target, relay, send_sem, recvs, relay_sem):
        arrived(relay, relay_sem)
        send(
            relay,
            target.at[chip(opposite)],
            send_sem,
            recvs.at[2],
            (base + chip(around), core),
        )

    eighth = CH // PIECES
    exchange = []
    for q in range(PIECES):
        piece = pl.ds(q * eighth, eighth)
        copy = send(
            own_ref.at[piece], other.at[piece], pair_send.at[q], pair_recv.at[q], partner
        )
        exchange.append(copy)

    def whiten(j):
        def pair_of_channels(c):
            rhs = jnp.concatenate(
                [own_ref[c], other[c], own_ref[c + 1], other[c + 1]], axis=0
            )
            spectra = lax.dot_general(
                table_ref[core, j],
                rhs,
                (((1,), (1,)), ((), ())),
                preferred_element_type=jnp.float32,
            )
            for half in range(2):
                re = spectra[:PADDED, 128 * half : 128 * half + 128]
                im = spectra[PADDED:, 128 * half : 128 * half + 128]
                power = jnp.sum(re * re + im * im, axis=1, keepdims=True)
                scaling = lax.rsqrt(power / windows + epsilon)
                re_buf[pl.ds(c + half, PADDED, stride=CH), :] = re * scaling
                im_buf[pl.ds(c + half, PADDED, stride=CH), :] = im * scaling

        for q in range(PIECES):
            if j == 0:
                exchange[q].wait_recv()

            @pl.loop(0, eighth // 2, unroll=2)
            def _(pair):
                pair_of_channels(q * eighth + 2 * pair)

        for b in range(ROW):

            @pl.loop(0, PART)
            def _(f):
                here = pl.ds(pl.multiple_of((b * PART + f) * CH, CH), CH)
                white[j, b, f, :, 0:128] = re_buf[here, :].astype(jnp.bfloat16)
                white[j, b, f, :, 128:256] = im_buf[here, :].astype(jnp.bfloat16)

        spread(
            white.at[j],
            group.at[j],
            relayed.at[j],
            white_send.at[j],
            white_recv.at[j],
            relay_recv.at[j],
        )

    def forward_white(j):
        forward(
            group.at[j], relayed.at[j], forward_send.at[j], white_recv.at[j], relay_recv.at[j]
        )

    halos = {}

    def send_halo(j):
        for b in range(2):
            arrived(group.at[j, b], white_recv.at[j, lax.rem(b + ROW - x, ROW)])
            halos[j, b] = send(
                group.at[j, b],
                halo.at[j, b],
                halo_send.at[j, b],
                halo_recv.at[j, b],
                (before, core),
            )

    last = row == rows - 1

    def correlate(j):
        for b in range(2, ROW):
            arrived(group.at[j, b], white_recv.at[j, lax.rem(b + ROW - x, ROW)])
        for b in range(2):
            halos[j, b].wait_recv()

        @pl.loop(0, PART)
        def _(f):
            blocks = [group[j, b, f] for b in range(ROW)]
            for b in range(2):
                there = halo[j, b, f]
                blocks.append(jnp.where(last, jnp.zeros_like(there), there))
            for b in range(ROW):
                mine = blocks[b]
                flipped = jnp.concatenate([mine[:, 128:], -mine[:, :128]], axis=1)
                lhs = jnp.concatenate([mine, flipped], axis=0)
                rhs = jnp.concatenate([*blocks[b : b + 3], mine], axis=0)
                product = lax.dot_general(
                    lhs, rhs, (((1,), (1,)), ((), ())), preferred_element_type=jnp.float32
                )
                for part in range(2):
                    cross[j, b, 2 * f + part] = skewed(product[32 * part : 32 * part + 32])

        spread(
            cross.at[j],
            back.at[j],
            cross_relayed.at[j],
            cross_send.at[j],
            cross_recv.at[j],
            cross_relay_recv.at[j],
        )

    def forward_cross(j):
        forward(
            back.at[j],
            cross_relayed.at[j],
            cross_forward_send.at[j],
            cross_recv.at[j],
            cross_relay_recv.at[j],
        )

    def turn(j):
        for b in range(ROW):
            arrived(back.at[j, b], cross_recv.at[j, lax.rem(b + ROW - x, ROW)])
        for b in range(ROW):

            @pl.loop(0, 2 * PART, unroll=2)
            def _(g):
                place = (j * ROW + b) * 2 * PART + g
                turned[pl.ds(place, 16, stride=CHUNKS * TERMS), :] = back[j, b, g].astype(
                    jnp.float32
                )

    whiten(0)
    whiten(1)
    whiten(2)
    forward_white(0)
    send_halo(0)
    forward_white(1)
    send_halo(1)
    forward_white(2)
    correlate(0)
    send_halo(2)
    correlate(1)
    forward_cross(0)
    turn(0)
    correlate(2)
    forward_cross(1)
    forward_cross(2)
    turn(1)
    turn(2)

    outs = []
    quarter = 16 // PIECES
    for q in range(PIECES):

        @pl.loop(q * quarter, (q + 1) * quarter, unroll=2)
        def _(p):
            c = 8 * (p // 8) + 7 - p % 8
            here = pl.ds(pl.multiple_of(p * CHUNKS * TERMS, 8), CHUNKS * TERMS)
            lags = lax.dot_general(
                turned[here, :].astype(jnp.bfloat16),
                inverse_ref[core],
                (((0,), (0,)), ((), ())),
                preferred_element_type=jnp.float32,
            )
            mine_out[p] = lags.astype(jnp.bfloat16)
            out_ref[c] = lags[:OFFS]
            out_ref[c + 16] = lags[OFFS:]

        piece = pl.ds(q * quarter, quarter)
        outs.append(
            send(mine_out.at[piece], theirs_in.at[piece], out_send.at[q], out_recv.at[q], partner)
        )

    sign = (1 - 2 * core).astype(jnp.float32)
    for q in range(PIECES):
        outs[q].wait_recv()

        @pl.loop(q * quarter, (q + 1) * quarter)
        def _(p):
            c = 8 * (p // 8) + 7 - p % 8
            theirs = theirs_in[p].astype(jnp.float32)
            out_ref[c] = sign * out_ref[c] + theirs[:OFFS]
            out_ref[c + 16] = sign * out_ref[c + 16] + theirs[OFFS:]

    for copy in sent:
        copy.wait_send()


VMEM = pl.BlockSpec(memory_space=pltpu.VMEM)


def body(rows, records):
    samples, channels, windows = records.shape
    assert (samples, channels) == (SAMPLES, CH)
    total_windows = 2 * windows
    own = jnp.transpose(records, (1, 2, 0))
    tables = np.stack(
        [[forward_table(parity, chunk) for chunk in range(CHUNKS)] for parity in range(2)]
    )
    factor = 1.0 / math.sqrt(2.0 * total_windows * (samples // 2 + 1))
    inverses = np.stack(
        [
            np.concatenate([inverse_table(parity, chunk, factor) for chunk in range(CHUNKS)])
            for parity in range(2)
        ]
    )
    bf16, f32 = jnp.bfloat16, jnp.float32
    dma = pltpu.SemaphoreType.DMA
    return pl.pallas_call(
        functools.partial(kernel, rows, total_windows),
        out_shape=jax.ShapeDtypeStruct((CH, OFFS, LAGS), f32),
        in_specs=[VMEM] * 3,
        out_specs=VMEM,
        scratch_shapes=[
            pltpu.VMEM((CH, windows, SAMPLES), bf16),
            pltpu.VMEM((PADDED * CH, 128), f32),
            pltpu.VMEM((PADDED * CH, 128), f32),
            pltpu.VMEM((CHUNKS, ROW, PART, CH, 256), bf16),
            pltpu.VMEM((CHUNKS, ROW, PART, CH, 256), bf16),
            pltpu.VMEM((CHUNKS, PART, CH, 256), bf16),
            pltpu.VMEM((CHUNKS, 2, PART, CH, 256), bf16),
            pltpu.VMEM((CHUNKS, ROW, 2 * PART, 16, 128), bf16),
            pltpu.VMEM((CHUNKS, 2 * PART, 16, 128), bf16),
            pltpu.VMEM((CHUNKS, ROW, 2 * PART, 16, 128), bf16),
            pltpu.VMEM((16 * CHUNKS * TERMS, 128), f32),
            pltpu.VMEM((16, 2 * OFFS, LAGS), bf16),
            pltpu.VMEM((16, 2 * OFFS, LAGS), bf16),
            dma((PIECES,)),
            dma((PIECES,)),
            dma((CHUNKS, 4)),
            dma((CHUNKS, 4)),
            dma((CHUNKS,)),
            dma((CHUNKS,)),
            dma((CHUNKS, 2)),
            dma((CHUNKS, 2)),
            dma((CHUNKS, 4)),
            dma((CHUNKS, 4)),
            dma((CHUNKS,)),
            dma((CHUNKS,)),
            dma((PIECES,)),
            dma((PIECES,)),
        ],
        compiler_params=pltpu.CompilerParams(collective_id=0, has_side_effects=True),
        name="correlate",
    )(tables, inverses, own)


def solution(mesh):
    rows = mesh.shape["cable"] // ROW
    return jax.shard_map(
        functools.partial(body, rows),
        mesh=mesh,
        in_specs=(P(None, "cable", "win"),),
        out_specs=P("cable", None, "win"),
        check_vma=False,
    )
```

```python
import functools
import math

import jax
import jax.numpy as jnp
import numpy as np
from jax import lax
from jax.experimental import pallas as pl
from jax.experimental.pallas import tpu as pltpu
from jax.sharding import PartitionSpec as P

MESH = pl.DeviceIdType.MESH

OFFS = 64
SAMPLES = 512
CH = 32
ROW = 4
CHUNKS = 3
PART = 11
FREQS = ROW * PART
PADDED = 48
TERMS = 2 * FREQS
LAGS = 256
PIECES = 4

epsilon = 1e-06
UNROLL = 4


def chunk_frequencies(parity, chunk):
    place = np.arange(PADDED)
    chip, slot = place // PART, chunk * PART + place % PART
    half = np.where(slot < 32, 32 * chip + slot, 128)
    held = np.where(slot < 32, chip < ROW, (chip == ROW - 1) & (parity == 0))
    return (2 * half + parity)[:, None], held[:, None]


def angles(freq, times):
    return np.float32(2.0 * math.pi / SAMPLES) * (freq * times % SAMPLES).astype(np.float32)


def forward_table(parity, chunk):
    freq, held = chunk_frequencies(parity, chunk)
    times = np.arange(SAMPLES)[None, :]
    phase = angles(freq, times)
    taper = np.float32(0.5) - np.float32(0.5) * np.cos(angles(1, times))
    taper = np.where(held, taper, np.float32(0.0))
    both = np.concatenate([taper * np.cos(phase), -taper * np.sin(phase)], axis=0)
    return both.astype(jnp.bfloat16)


def inverse_table(parity, chunk, factor):
    freq, held = chunk_frequencies(parity, chunk)
    freq, held = freq[:FREQS], held[:FREQS]
    phase = angles(freq, np.arange(LAGS)[None, :])
    weight = np.where((freq == 0) | (freq == SAMPLES // 2), 1.0, 2.0) * held * factor
    weight = weight.astype(np.float32)
    both = np.stack([weight * np.cos(phase), -weight * np.sin(phase)], axis=1)
    return both.reshape(TERMS, LAGS).astype(jnp.bfloat16)


def skewed(product):
    lane = lax.broadcasted_iota(jnp.int32, (8, 128), 1)
    back = 7 - lax.broadcasted_iota(jnp.int32, (8, 128), 0)
    turned = []
    for v in range(4):
        group = jnp.take_along_axis(product[8 * v : 8 * v + 8], back, axis=0)
        shift = (120 - 8 * v + 64 * (v // 2)) % 128
        turned.append(pltpu.roll(group, shift, 1, stride=1, stride_axis=0))
    both = [jnp.where(lane < OFFS, turned[v], turned[v + 2]) for v in range(2)]
    return jnp.concatenate(both, axis=0).astype(jnp.bfloat16)


def kernel(
    rows,
    windows,
    table_ref,
    inverse_ref,
    own_ref,
    out_ref,
    theirs_ref,
    other,
    re_buf,
    im_buf,
    white,
    group,
    halo,
    cross,
    back,
    turned,
    mine_out,
    pair_send,
    pair_recv,
    white_send,
    white_recv,
    halo_send,
    halo_recv,
    cross_send,
    cross_recv,
    out_send,
    out_recv,
):
    me = lax.axis_index("cable")
    core = lax.axis_index("win")
    x, row = lax.rem(me, ROW), lax.div(me, ROW)
    base = row * ROW

    def chip(distance):
        return lax.rem(x + distance, ROW)

    before = lax.rem(row + rows - 1, rows) * ROW + x
    after = lax.rem(row + 1, rows) * ROW + x
    partner = (me, 1 - core)
    barrier = pltpu.get_barrier_semaphore()
    for device in [
        partner,
        (base + chip(1), core),
        (base + chip(2), core),
        (base + chip(3), core),
        (before, core),
        (after, core),
    ]:
        pl.semaphore_signal(barrier, inc=1, device_id=device, device_id_type=MESH)
    pl.semaphore_wait(barrier, 6)

    sent = []

    def copy_to(source, target, send_sem, recv_sem, device):
        return pltpu.make_async_remote_copy(
            src_ref=source,
            dst_ref=target,
            send_sem=send_sem,
            recv_sem=recv_sem,
            device_id=device,
            device_id_type=MESH,
        )

    def send(*args):
        copy = copy_to(*args)
        copy.start()
        sent.append(copy)
        return copy

    def arrived(target, sem):
        pltpu.make_async_copy(target, target, sem).wait()

    def spread(source, target, sends, recvs):
        for distance in (2, 1, 3):
            send(
                source.at[chip(distance)],
                target.at[x],
                sends.at[distance],
                recvs.at[4 - distance],
                (base + chip(distance), core),
            )
        pltpu.make_async_copy(source.at[x], target.at[x], recvs.at[0]).start()

    eighth = CH // PIECES
    exchange = []
    for q in range(PIECES):
        piece = pl.ds(q * eighth, eighth)
        copy = send(
            own_ref.at[piece], other.at[piece], pair_send.at[q], pair_recv.at[q], partner
        )
        exchange.append(copy)

    def whiten(j):
        def pair_of_channels(c):
            rhs = jnp.concatenate(
                [own_ref[c], other[c], own_ref[c + 1], other[c + 1]], axis=0
            )
            spectra = lax.dot_general(
                table_ref[core, j],
                rhs,
                (((1,), (1,)), ((), ())),
                preferred_element_type=jnp.float32,
            )
            for half in range(2):
                re = spectra[:PADDED, 128 * half : 128 * half + 128]
                im = spectra[PADDED:, 128 * half : 128 * half + 128]
                power = jnp.sum(re * re + im * im, axis=1, keepdims=True)
                scaling = lax.rsqrt(power / windows + epsilon)
                re_buf[pl.ds(c + half, PADDED, stride=CH), :] = re * scaling
                im_buf[pl.ds(c + half, PADDED, stride=CH), :] = im * scaling

        for q in range(PIECES):
            if j == 0:
                exchange[q].wait_recv()

            @pl.loop(0, eighth // 2, unroll=4)
            def _(pair):
                pair_of_channels(q * eighth + 2 * pair)

        for b in range(ROW):

            @pl.loop(0, PART)
            def _(f):
                here = pl.ds(pl.multiple_of((b * PART + f) * CH, CH), CH)
                white[j, b, f, :, 0:128] = re_buf[here, :].astype(jnp.bfloat16)
                white[j, b, f, :, 128:256] = im_buf[here, :].astype(jnp.bfloat16)

    def send_white(j):
        spread(white.at[j], group.at[j], white_send.at[j], white_recv.at[j])

    halos = {}

    def send_halo(j):
        for b in range(2):
            arrived(group.at[j, b], white_recv.at[j, lax.rem(b + ROW - x, ROW)])
            halos[j, b] = send(
                group.at[j, b],
                halo.at[j, b],
                halo_send.at[j, b],
                halo_recv.at[j, b],
                (before, core),
            )

    last = row == rows - 1

    def correlate(j):
        for b in range(2, ROW):
            arrived(group.at[j, b], white_recv.at[j, lax.rem(b + ROW - x, ROW)])
        for b in range(2):
            halos[j, b].wait_recv()

        @pl.loop(0, PART)
        def _(f):
            for b in range(ROW):
                mine = group[j, b, f]
                flipped = jnp.concatenate([mine[:, 128:], -mine[:, :128]], axis=1)
                lhs = jnp.concatenate([mine, flipped], axis=0)
                partners = []
                for other_block in range(b, b + 3):
                    if other_block < ROW:
                        partners.append(group[j, other_block, f])
                    else:
                        there = halo[j, other_block - ROW, f]
                        partners.append(jnp.where(last, jnp.zeros_like(there), there))
                rhs = jnp.concatenate([*partners, mine], axis=0)
                product = lax.dot_general(
                    lhs, rhs, (((1,), (1,)), ((), ())), preferred_element_type=jnp.float32
                )
                for part in range(2):
                    cross[j, b, 2 * f + part] = skewed(product[32 * part : 32 * part + 32])

        spread(cross.at[j], back.at[j], cross_send.at[j], cross_recv.at[j])

    outs = []
    quarter = 16 // PIECES

    def turn(j):
        for b in range(ROW):
            arrived(back.at[j, b], cross_recv.at[j, lax.rem(b + ROW - x, ROW)])
        for b in range(ROW):

            @pl.loop(0, 2 * PART, unroll=2)
            def _(g):
                turned[pl.ds(b * 2 * PART + g, 16, stride=TERMS), :] = back[j, b, g].astype(
                    jnp.float32
                )

        for q in range(PIECES):

            @pl.loop(q * quarter, (q + 1) * quarter, unroll=UNROLL)
            def _(p):
                c = 8 * (p // 8) + 7 - p % 8
                here = pl.ds(pl.multiple_of(p * TERMS, 8), TERMS)
                lags = lax.dot_general(
                    turned[here, :].astype(jnp.bfloat16),
                    inverse_ref[core, j],
                    (((0,), (0,)), ((), ())),
                    preferred_element_type=jnp.float32,
                )
                for half in range(2):
                    total = lags[OFFS * half : OFFS * half + OFFS]
                    if j > 0:
                        total = total + out_ref[c + 16 * half]
                    out_ref[c + 16 * half] = total
                    if j == CHUNKS - 1:
                        mine_out[c + 16 * half] = total.astype(jnp.bfloat16)

            if j == CHUNKS - 1:
                for half in range(2):
                    first = 8 * (q // 2) + 4 * (1 - q % 2) + 16 * half
                    piece = pl.ds(first, quarter)
                    place = 2 * q + half
                    outs.append(
                        send(
                            mine_out.at[piece],
                            theirs_ref.at[piece],
                            out_send.at[place],
                            out_recv.at[place],
                            partner,
                        )
                    )

    whiten(0)
    send_white(0)
    whiten(1)
    send_white(1)
    whiten(2)
    send_white(2)
    send_halo(0)
    send_halo(1)
    correlate(0)
    send_halo(2)
    correlate(1)
    correlate(2)
    turn(0)
    turn(1)
    turn(2)

    for copy in outs:
        copy.wait_recv()
    for copy in sent:
        copy.wait_send()


VMEM = pl.BlockSpec(memory_space=pltpu.VMEM)


def body(rows, records):
    samples, channels, windows = records.shape
    assert (samples, channels) == (SAMPLES, CH)
    total_windows = 2 * windows
    own = jnp.transpose(records, (1, 2, 0))
    tables = np.stack(
        [[forward_table(parity, chunk) for chunk in range(CHUNKS)] for parity in range(2)]
    )
    factor = 1.0 / math.sqrt(2.0 * total_windows * (samples // 2 + 1))
    inverses = np.stack(
        [
            [inverse_table(parity, chunk, factor) for chunk in range(CHUNKS)]
            for parity in range(2)
        ]
    )
    bf16, f32 = jnp.bfloat16, jnp.float32
    dma = pltpu.SemaphoreType.DMA
    half, theirs = pl.pallas_call(
        functools.partial(kernel, rows, total_windows),
        out_shape=[
            jax.ShapeDtypeStruct((CH, OFFS, LAGS), f32),
            jax.ShapeDtypeStruct((CH, OFFS, LAGS), bf16),
        ],
        in_specs=[VMEM] * 3,
        out_specs=[VMEM] * 2,
        scratch_shapes=[
            pltpu.VMEM((CH, windows, SAMPLES), bf16),
            pltpu.VMEM((PADDED * CH, 128), f32),
            pltpu.VMEM((PADDED * CH, 128), f32),
            pltpu.VMEM((CHUNKS, ROW, PART, CH, 256), bf16),
            pltpu.VMEM((CHUNKS, ROW, PART, CH, 256), bf16),
            pltpu.VMEM((CHUNKS, 2, PART, CH, 256), bf16),
            pltpu.VMEM((CHUNKS, ROW, 2 * PART, 16, 128), bf16),
            pltpu.VMEM((CHUNKS, ROW, 2 * PART, 16, 128), bf16),
            pltpu.VMEM((16 * TERMS, 128), f32),
            pltpu.VMEM((CH, OFFS, LAGS), bf16),
            dma((PIECES,)),
            dma((PIECES,)),
            dma((CHUNKS, 4)),
            dma((CHUNKS, 4)),
            dma((CHUNKS, 2)),
            dma((CHUNKS, 2)),
            dma((CHUNKS, 4)),
            dma((CHUNKS, 4)),
            dma((2 * PIECES,)),
            dma((2 * PIECES,)),
        ],
        compiler_params=pltpu.CompilerParams(collective_id=0, has_side_effects=True),
        name="correlate",
    )(tables, inverses, own)
    return jnp.where(lax.axis_index("win") == 0, half, -half) + theirs.astype(f32)


def solution(mesh):
    rows = mesh.shape["cable"] // ROW
    return jax.shard_map(
        functools.partial(body, rows),
        mesh=mesh,
        in_specs=(P(None, "cable", "win"),),
        out_specs=P("cable", None, "win"),
        check_vma=False,
    )
```

```python
import functools
import math

import jax
import jax.numpy as jnp
import numpy as np
from jax import lax
from jax.experimental import pallas as pl
from jax.experimental.pallas import tpu as pltpu
from jax.sharding import PartitionSpec as P

MESH = pl.DeviceIdType.MESH

OFFS = 64
SAMPLES = 512
CH = 32
ROW = 4
CHUNKS = 3
PART = 11
FREQS = ROW * PART
PADDED = 48
TERMS = 2 * FREQS
LAGS = 256
PIECES = 4

epsilon = 1e-06
UNROLL = 4


def chunk_frequencies(parity, chunk):
    place = np.arange(PADDED)
    chip, slot = place // PART, chunk * PART + place % PART
    half = np.where(slot < 32, 32 * chip + slot, 128)
    held = np.where(slot < 32, chip < ROW, (chip == ROW - 1) & (parity == 0))
    return (2 * half + parity)[:, None], held[:, None]


def angles(freq, times):
    return np.float32(2.0 * math.pi / SAMPLES) * (freq * times % SAMPLES).astype(np.float32)


def forward_table(parity, chunk):
    freq, held = chunk_frequencies(parity, chunk)
    times = np.arange(SAMPLES)[None, :]
    phase = angles(freq, times)
    taper = np.float32(0.5) - np.float32(0.5) * np.cos(angles(1, times))
    taper = np.where(held, taper, np.float32(0.0))
    both = np.concatenate([taper * np.cos(phase), -taper * np.sin(phase)], axis=0)
    return both.astype(jnp.bfloat16)


def inverse_table(parity, chunk, factor):
    freq, held = chunk_frequencies(parity, chunk)
    freq, held = freq[:FREQS], held[:FREQS]
    phase = angles(freq, np.arange(LAGS)[None, :])
    weight = np.where((freq == 0) | (freq == SAMPLES // 2), 1.0, 2.0) * held * factor
    weight = weight.astype(np.float32)
    both = np.stack([weight * np.cos(phase), -weight * np.sin(phase)], axis=1)
    return both.reshape(TERMS, LAGS).astype(jnp.bfloat16)


def skewed(product):
    lane = lax.broadcasted_iota(jnp.int32, (8, 128), 1)
    back = 7 - lax.broadcasted_iota(jnp.int32, (8, 128), 0)
    turned = []
    for v in range(4):
        group = jnp.take_along_axis(product[8 * v : 8 * v + 8], back, axis=0)
        shift = (120 - 8 * v + 64 * (v // 2)) % 128
        turned.append(pltpu.roll(group, shift, 1, stride=1, stride_axis=0))
    both = [jnp.where(lane < OFFS, turned[v], turned[v + 2]) for v in range(2)]
    return jnp.concatenate(both, axis=0).astype(jnp.bfloat16)


def kernel(
    rows,
    windows,
    table_ref,
    inverse_ref,
    own_ref,
    half_ref,
    theirs_ref,
    out_ref,
    other,
    re_buf,
    im_buf,
    white,
    group,
    halo,
    cross,
    back,
    turned,
    pair_send,
    pair_recv,
    white_send,
    white_recv,
    halo_send,
    halo_recv,
    cross_send,
    cross_recv,
    out_send,
    out_recv,
):
    me = lax.axis_index("cable")
    core = lax.axis_index("win")
    x, row = lax.rem(me, ROW), lax.div(me, ROW)
    base = row * ROW

    def chip(distance):
        return lax.rem(x + distance, ROW)

    before = lax.rem(row + rows - 1, rows) * ROW + x
    after = lax.rem(row + 1, rows) * ROW + x
    partner = (me, 1 - core)
    barrier = pltpu.get_barrier_semaphore()
    for device in [
        partner,
        (base + chip(1), core),
        (base + chip(2), core),
        (base + chip(3), core),
        (before, core),
        (after, core),
    ]:
        pl.semaphore_signal(barrier, inc=1, device_id=device, device_id_type=MESH)
    pl.semaphore_wait(barrier, 6)

    sent = []

    def copy_to(source, target, send_sem, recv_sem, device):
        return pltpu.make_async_remote_copy(
            src_ref=source,
            dst_ref=target,
            send_sem=send_sem,
            recv_sem=recv_sem,
            device_id=device,
            device_id_type=MESH,
        )

    def send(*args):
        copy = copy_to(*args)
        copy.start()
        sent.append(copy)
        return copy

    def arrived(target, sem):
        pltpu.make_async_copy(target, target, sem).wait()

    def spread(source, target, sends, recvs):
        for distance in (2, 1, 3):
            send(
                source.at[chip(distance)],
                target.at[x],
                sends.at[distance],
                recvs.at[4 - distance],
                (base + chip(distance), core),
            )
        pltpu.make_async_copy(source.at[x], target.at[x], recvs.at[0]).start()

    eighth = CH // PIECES
    exchange = []
    for q in range(PIECES):
        piece = pl.ds(q * eighth, eighth)
        copy = send(
            own_ref.at[piece], other.at[piece], pair_send.at[q], pair_recv.at[q], partner
        )
        exchange.append(copy)

    def whiten(j):
        def pair_of_channels(c):
            rhs = jnp.concatenate(
                [own_ref[c], other[c], own_ref[c + 1], other[c + 1]], axis=0
            )
            spectra = lax.dot_general(
                table_ref[core, j],
                rhs,
                (((1,), (1,)), ((), ())),
                preferred_element_type=jnp.float32,
            )
            for half in range(2):
                re = spectra[:PADDED, 128 * half : 128 * half + 128]
                im = spectra[PADDED:, 128 * half : 128 * half + 128]
                power = jnp.sum(re * re + im * im, axis=1, keepdims=True)
                scaling = lax.rsqrt(power / windows + epsilon)
                re_buf[pl.ds(c + half, PADDED, stride=CH), :] = re * scaling
                im_buf[pl.ds(c + half, PADDED, stride=CH), :] = im * scaling

        for q in range(PIECES):
            if j == 0:
                exchange[q].wait_recv()

            @pl.loop(0, eighth // 2, unroll=4)
            def _(pair):
                pair_of_channels(q * eighth + 2 * pair)

        for b in range(ROW):

            @pl.loop(0, PART, unroll=PART)
            def _(f):
                here = pl.ds(pl.multiple_of((b * PART + f) * CH, CH), CH)
                white[j, b, f, :, 0:128] = re_buf[here, :].astype(jnp.bfloat16)
                white[j, b, f, :, 128:256] = im_buf[here, :].astype(jnp.bfloat16)

    def send_white(j):
        spread(white.at[j], group.at[j], white_send.at[j], white_recv.at[j])

    halos = {}

    def send_halo(j):
        for b in range(2):
            arrived(group.at[j, b], white_recv.at[j, lax.rem(b + ROW - x, ROW)])
            halos[j, b] = send(
                group.at[j, b],
                halo.at[j, b],
                halo_send.at[j, b],
                halo_recv.at[j, b],
                (before, core),
            )

    last = row == rows - 1

    def correlate(j):
        for b in range(2, ROW):
            arrived(group.at[j, b], white_recv.at[j, lax.rem(b + ROW - x, ROW)])
        for b in range(2):
            halos[j, b].wait_recv()

        def frequency(f):
            for b in range(ROW):
                mine = group[j, b, f]
                flipped = jnp.concatenate([mine[:, 128:], -mine[:, :128]], axis=1)
                lhs = jnp.concatenate([mine, flipped], axis=0)
                partners = []
                for other_block in range(b, b + 3):
                    if other_block < ROW:
                        partners.append(group[j, other_block, f])
                    else:
                        there = halo[j, other_block - ROW, f]
                        partners.append(jnp.where(last, jnp.zeros_like(there), there))
                rhs = jnp.concatenate([*partners, mine], axis=0)
                product = lax.dot_general(
                    lhs, rhs, (((1,), (1,)), ((), ())), preferred_element_type=jnp.float32
                )
                for part in range(2):
                    cross[j, b, 2 * f + part] = skewed(product[32 * part : 32 * part + 32])

        @pl.loop(0, PART // 2)
        def _(pair):
            frequency(2 * pair)
            frequency(2 * pair + 1)

        frequency(PART - 1)

        spread(cross.at[j], back.at[j], cross_send.at[j], cross_recv.at[j])

    outs = []
    quarter = 16 // PIECES

    def turn(j):
        for b in range(ROW):
            arrived(back.at[j, b], cross_recv.at[j, lax.rem(b + ROW - x, ROW)])
        for b in range(ROW):

            @pl.loop(0, 2 * PART, unroll=PART)
            def _(g):
                turned[pl.ds(b * 2 * PART + g, 16, stride=TERMS), :] = back[j, b, g].astype(
                    jnp.float32
                )

        for q in range(PIECES):

            @pl.loop(q * quarter, (q + 1) * quarter, unroll=UNROLL)
            def _(p):
                c = 8 * (p // 8) + 7 - p % 8
                here = pl.ds(pl.multiple_of(p * TERMS, 8), TERMS)
                lags = lax.dot_general(
                    turned[here, :].astype(jnp.bfloat16),
                    inverse_ref[core, j],
                    (((0,), (0,)), ((), ())),
                    preferred_element_type=jnp.float32,
                )
                for half in range(2):
                    total = lags[OFFS * half : OFFS * half + OFFS]
                    if j > 0:
                        total = total + out_ref[c + 16 * half]
                    if j < CHUNKS - 1:
                        out_ref[c + 16 * half] = total
                    else:
                        half_ref[c + 16 * half] = total.astype(jnp.bfloat16)

            if j == CHUNKS - 1:
                for half in range(2):
                    first = 8 * (q // 2) + 4 * (1 - q % 2) + 16 * half
                    piece = pl.ds(first, quarter)
                    place = 2 * q + half
                    outs.append(
                        send(
                            half_ref.at[piece],
                            theirs_ref.at[piece],
                            out_send.at[place],
                            out_recv.at[place],
                            partner,
                        )
                    )

    whiten(0)
    send_white(0)
    whiten(1)
    send_white(1)
    whiten(2)
    send_white(2)
    send_halo(0)
    send_halo(1)
    correlate(0)
    send_halo(2)
    correlate(1)
    correlate(2)
    turn(0)
    turn(1)
    turn(2)

    for copy in outs:
        copy.wait_recv()
    for copy in sent:
        copy.wait_send()


VMEM = pl.BlockSpec(memory_space=pltpu.VMEM)


def body(rows, records):
    samples, channels, windows = records.shape
    assert (samples, channels) == (SAMPLES, CH)
    total_windows = 2 * windows
    own = jnp.transpose(records, (1, 2, 0))
    tables = np.stack(
        [[forward_table(parity, chunk) for chunk in range(CHUNKS)] for parity in range(2)]
    )
    factor = 1.0 / math.sqrt(2.0 * total_windows * (samples // 2 + 1))
    inverses = np.stack(
        [
            [inverse_table(parity, chunk, factor) for chunk in range(CHUNKS)]
            for parity in range(2)
        ]
    )
    bf16, f32 = jnp.bfloat16, jnp.float32
    dma = pltpu.SemaphoreType.DMA
    half, theirs = pl.pallas_call(
        functools.partial(kernel, rows, total_windows),
        out_shape=[
            jax.ShapeDtypeStruct((CH, OFFS, LAGS), bf16),
            jax.ShapeDtypeStruct((CH, OFFS, LAGS), bf16),
        ],
        in_specs=[VMEM] * 3,
        out_specs=[VMEM] * 2,
        scratch_shapes=[
            pltpu.VMEM((CH, OFFS, LAGS), f32),
            pltpu.VMEM((CH, windows, SAMPLES), bf16),
            pltpu.VMEM((PADDED * CH, 128), f32),
            pltpu.VMEM((PADDED * CH, 128), f32),
            pltpu.VMEM((CHUNKS, ROW, PART, CH, 256), bf16),
            pltpu.VMEM((CHUNKS, ROW, PART, CH, 256), bf16),
            pltpu.VMEM((CHUNKS, 2, PART, CH, 256), bf16),
            pltpu.VMEM((CHUNKS, ROW, 2 * PART, 16, 128), bf16),
            pltpu.VMEM((CHUNKS, ROW, 2 * PART, 16, 128), bf16),
            pltpu.VMEM((16 * TERMS, 128), f32),
            dma((PIECES,)),
            dma((PIECES,)),
            dma((CHUNKS, 4)),
            dma((CHUNKS, 4)),
            dma((CHUNKS, 2)),
            dma((CHUNKS, 2)),
            dma((CHUNKS, 4)),
            dma((CHUNKS, 4)),
            dma((2 * PIECES,)),
            dma((2 * PIECES,)),
        ],
        compiler_params=pltpu.CompilerParams(collective_id=0, has_side_effects=True),
        name="correlate",
    )(tables, inverses, own)
    half = half.astype(f32)
    return jnp.where(lax.axis_index("win") == 0, half, -half) + theirs.astype(f32)


def solution(mesh):
    rows = mesh.shape["cable"] // ROW
    return jax.shard_map(
        functools.partial(body, rows),
        mesh=mesh,
        in_specs=(P(None, "cable", "win"),),
        out_specs=P("cable", None, "win"),
        check_vma=False,
    )
```

```python
import functools
import math

import jax
import jax.numpy as jnp
import numpy as np
from jax import lax
from jax.experimental import pallas as pl
from jax.experimental.pallas import tpu as pltpu
from jax.sharding import PartitionSpec as P

MESH = pl.DeviceIdType.MESH

OFFS = 64
SAMPLES = 512
CH = 32
ROW = 4
CHUNKS = 3
PART = 11
FREQS = ROW * PART
PADDED = 48
TERMS = 2 * FREQS
LAGS = 256
SPANS = ((0, 6), (6, 5))
PIECES = 4

epsilon = 1e-06
UNROLL = 4


def chunk_frequencies(parity, chunk):
    place = np.arange(PADDED)
    chip, slot = place // PART, chunk * PART + place % PART
    half = np.where(slot < 32, 32 * chip + slot, 128)
    held = np.where(slot < 32, chip < ROW, (chip == ROW - 1) & (parity == 0))
    return (2 * half + parity)[:, None], held[:, None]


def angles(freq, times):
    return np.float32(2.0 * math.pi / SAMPLES) * (freq * times % SAMPLES).astype(np.float32)


def forward_table(parity, chunk):
    freq, held = chunk_frequencies(parity, chunk)
    times = np.arange(SAMPLES)[None, :]
    phase = angles(freq, times)
    taper = np.float32(0.5) - np.float32(0.5) * np.cos(angles(1, times))
    taper = np.where(held, taper, np.float32(0.0))
    both = np.concatenate([taper * np.cos(phase), -taper * np.sin(phase)], axis=0)
    return both.astype(jnp.bfloat16)


def inverse_table(parity, chunk, factor):
    freq, held = chunk_frequencies(parity, chunk)
    freq, held = freq[:FREQS], held[:FREQS]
    phase = angles(freq, np.arange(LAGS)[None, :])
    weight = np.where((freq == 0) | (freq == SAMPLES // 2), 1.0, 2.0) * held * factor
    weight = weight.astype(np.float32)
    both = np.stack([weight * np.cos(phase), -weight * np.sin(phase)], axis=1)
    return both.reshape(TERMS, LAGS).astype(jnp.bfloat16)


def skewed(product):
    lane = lax.broadcasted_iota(jnp.int32, (8, 128), 1)
    back = 7 - lax.broadcasted_iota(jnp.int32, (8, 128), 0)
    turned = []
    for v in range(4):
        group = jnp.take_along_axis(product[8 * v : 8 * v + 8], back, axis=0)
        shift = (120 - 8 * v + 64 * (v // 2)) % 128
        turned.append(pltpu.roll(group, shift, 1, stride=1, stride_axis=0))
    both = [jnp.where(lane < OFFS, turned[v], turned[v + 2]) for v in range(2)]
    return jnp.concatenate(both, axis=0).astype(jnp.bfloat16)


def kernel(
    rows,
    windows,
    table_ref,
    inverse_ref,
    own_ref,
    half_ref,
    theirs_ref,
    out_ref,
    other,
    re_buf,
    im_buf,
    white,
    group,
    halo,
    cross,
    back,
    turned,
    pair_send,
    pair_recv,
    white_send,
    white_recv,
    halo_send,
    halo_recv,
    cross_send,
    cross_recv,
    out_send,
    out_recv,
):
    me = lax.axis_index("cable")
    core = lax.axis_index("win")
    x, row = lax.rem(me, ROW), lax.div(me, ROW)
    base = row * ROW

    def chip(distance):
        return lax.rem(x + distance, ROW)

    before = lax.rem(row + rows - 1, rows) * ROW + x
    after = lax.rem(row + 1, rows) * ROW + x
    partner = (me, 1 - core)
    barrier = pltpu.get_barrier_semaphore()
    for device in [
        partner,
        (base + chip(1), core),
        (base + chip(2), core),
        (base + chip(3), core),
        (before, core),
        (after, core),
    ]:
        pl.semaphore_signal(barrier, inc=1, device_id=device, device_id_type=MESH)
    pl.semaphore_wait(barrier, 6)

    sent = []

    def copy_to(source, target, send_sem, recv_sem, device):
        return pltpu.make_async_remote_copy(
            src_ref=source,
            dst_ref=target,
            send_sem=send_sem,
            recv_sem=recv_sem,
            device_id=device,
            device_id_type=MESH,
        )

    def send(*args):
        copy = copy_to(*args)
        copy.start()
        sent.append(copy)
        return copy

    def arrived(target, sem):
        pltpu.make_async_copy(target, target, sem).wait()

    def spread(source, target, sends, recvs):
        for distance in (2, 1, 3):
            send(
                source.at[chip(distance)],
                target.at[x],
                sends.at[distance],
                recvs.at[4 - distance],
                (base + chip(distance), core),
            )
        pltpu.make_async_copy(source.at[x], target.at[x], recvs.at[0]).start()

    eighth = CH // PIECES
    exchange = []
    for q in range(PIECES):
        piece = pl.ds(q * eighth, eighth)
        copy = send(
            own_ref.at[piece], other.at[piece], pair_send.at[q], pair_recv.at[q], partner
        )
        exchange.append(copy)

    def whiten(j):
        def pair_of_channels(c):
            rhs = jnp.concatenate(
                [own_ref[c], other[c], own_ref[c + 1], other[c + 1]], axis=0
            )
            spectra = lax.dot_general(
                table_ref[core, j],
                rhs,
                (((1,), (1,)), ((), ())),
                preferred_element_type=jnp.float32,
            )
            for half in range(2):
                re = spectra[:PADDED, 128 * half : 128 * half + 128]
                im = spectra[PADDED:, 128 * half : 128 * half + 128]
                power = jnp.sum(re * re + im * im, axis=1, keepdims=True)
                scaling = lax.rsqrt(power / windows + epsilon)
                re_buf[pl.ds(c + half, PADDED, stride=CH), :] = re * scaling
                im_buf[pl.ds(c + half, PADDED, stride=CH), :] = im * scaling

        for q in range(PIECES):
            if j == 0:
                exchange[q].wait_recv()

            @pl.loop(0, eighth // 2, unroll=4)
            def _(pair):
                pair_of_channels(q * eighth + 2 * pair)

        for b in range(ROW):

            @pl.loop(0, PART, unroll=PART)
            def _(f):
                here = pl.ds(pl.multiple_of((b * PART + f) * CH, CH), CH)
                white[j, b, f, :, 0:128] = re_buf[here, :].astype(jnp.bfloat16)
                white[j, b, f, :, 128:256] = im_buf[here, :].astype(jnp.bfloat16)

    def send_white(j):
        spread(white.at[j], group.at[j], white_send.at[j], white_recv.at[j])

    halos = {}

    def send_halo(j):
        for b in range(2):
            arrived(group.at[j, b], white_recv.at[j, lax.rem(b + ROW - x, ROW)])
            halos[j, b] = send(
                group.at[j, b],
                halo.at[j, b],
                halo_send.at[j, b],
                halo_recv.at[j, b],
                (before, core),
            )

    last = row == rows - 1

    def of_span(ref, span):
        first, size = SPANS[span]
        return ref.at[:, pl.ds(2 * first, 2 * size)]

    def correlate(j):
        for b in range(2, ROW):
            arrived(group.at[j, b], white_recv.at[j, lax.rem(b + ROW - x, ROW)])
        for b in range(2):
            halos[j, b].wait_recv()

        def frequency(f):
            for b in range(ROW):
                mine = group[j, b, f]
                flipped = jnp.concatenate([mine[:, 128:], -mine[:, :128]], axis=1)
                lhs = jnp.concatenate([mine, flipped], axis=0)
                partners = []
                for other_block in range(b, b + 3):
                    if other_block < ROW:
                        partners.append(group[j, other_block, f])
                    else:
                        there = halo[j, other_block - ROW, f]
                        partners.append(jnp.where(last, jnp.zeros_like(there), there))
                rhs = jnp.concatenate([*partners, mine], axis=0)
                product = lax.dot_general(
                    lhs, rhs, (((1,), (1,)), ((), ())), preferred_element_type=jnp.float32
                )
                for part in range(2):
                    cross[j, b, 2 * f + part] = skewed(product[32 * part : 32 * part + 32])

        for span, (first, size) in enumerate(SPANS):

            @pl.loop(0, size // 2)
            def _(pair):
                frequency(first + 2 * pair)
                frequency(first + 2 * pair + 1)

            if size % 2:
                frequency(first + size - 1)
            spread(
                of_span(cross.at[j], span),
                of_span(back.at[j], span),
                cross_send.at[j, span],
                cross_recv.at[j, span],
            )

    outs = []
    quarter = 16 // PIECES

    def turn(j):
        for span, (first, size) in enumerate(SPANS):
            for b in range(ROW):
                arrived(
                    back.at[j, b, pl.ds(2 * first, 2 * size)],
                    cross_recv.at[j, span, lax.rem(b + ROW - x, ROW)],
                )
            for b in range(ROW):

                @pl.loop(2 * first, 2 * (first + size), unroll=2 * size)
                def _(g):
                    turned[pl.ds(b * 2 * PART + g, 16, stride=TERMS), :] = back[j, b, g].astype(
                        jnp.float32
                    )

        for q in range(PIECES):

            @pl.loop(q * quarter, (q + 1) * quarter, unroll=UNROLL)
            def _(p):
                c = 8 * (p // 8) + 7 - p % 8
                here = pl.ds(pl.multiple_of(p * TERMS, 8), TERMS)
                lags = lax.dot_general(
                    turned[here, :].astype(jnp.bfloat16),
                    inverse_ref[core, j],
                    (((0,), (0,)), ((), ())),
                    preferred_element_type=jnp.float32,
                )
                for half in range(2):
                    total = lags[OFFS * half : OFFS * half + OFFS]
                    if j > 0:
                        total = total + out_ref[c + 16 * half]
                    if j < CHUNKS - 1:
                        out_ref[c + 16 * half] = total
                    else:
                        half_ref[c + 16 * half] = total.astype(jnp.bfloat16)

            if j == CHUNKS - 1:
                for half in range(2):
                    first = 8 * (q // 2) + 4 * (1 - q % 2) + 16 * half
                    piece = pl.ds(first, quarter)
                    place = 2 * q + half
                    outs.append(
                        send(
                            half_ref.at[piece],
                            theirs_ref.at[piece],
                            out_send.at[place],
                            out_recv.at[place],
                            partner,
                        )
                    )

    whiten(0)
    send_white(0)
    whiten(1)
    send_white(1)
    whiten(2)
    send_white(2)
    send_halo(0)
    send_halo(1)
    correlate(0)
    send_halo(2)
    correlate(1)
    correlate(2)
    turn(0)
    turn(1)
    turn(2)

    for copy in outs:
        copy.wait_recv()
    for copy in sent:
        copy.wait_send()


VMEM = pl.BlockSpec(memory_space=pltpu.VMEM)


def body(rows, records):
    samples, channels, windows = records.shape
    assert (samples, channels) == (SAMPLES, CH)
    total_windows = 2 * windows
    own = jnp.transpose(records, (1, 2, 0))
    tables = np.stack(
        [[forward_table(parity, chunk) for chunk in range(CHUNKS)] for parity in range(2)]
    )
    factor = 1.0 / math.sqrt(2.0 * total_windows * (samples // 2 + 1))
    inverses = np.stack(
        [
            [inverse_table(parity, chunk, factor) for chunk in range(CHUNKS)]
            for parity in range(2)
        ]
    )
    bf16, f32 = jnp.bfloat16, jnp.float32
    dma = pltpu.SemaphoreType.DMA
    half, theirs = pl.pallas_call(
        functools.partial(kernel, rows, total_windows),
        out_shape=[
            jax.ShapeDtypeStruct((CH, OFFS, LAGS), bf16),
            jax.ShapeDtypeStruct((CH, OFFS, LAGS), bf16),
        ],
        in_specs=[VMEM] * 3,
        out_specs=[VMEM] * 2,
        scratch_shapes=[
            pltpu.VMEM((CH, OFFS, LAGS), f32),
            pltpu.VMEM((CH, windows, SAMPLES), bf16),
            pltpu.VMEM((PADDED * CH, 128), f32),
            pltpu.VMEM((PADDED * CH, 128), f32),
            pltpu.VMEM((CHUNKS, ROW, PART, CH, 256), bf16),
            pltpu.VMEM((CHUNKS, ROW, PART, CH, 256), bf16),
            pltpu.VMEM((CHUNKS, 2, PART, CH, 256), bf16),
            pltpu.VMEM((CHUNKS, ROW, 2 * PART, 16, 128), bf16),
            pltpu.VMEM((CHUNKS, ROW, 2 * PART, 16, 128), bf16),
            pltpu.VMEM((16 * TERMS, 128), f32),
            dma((PIECES,)),
            dma((PIECES,)),
            dma((CHUNKS, 4)),
            dma((CHUNKS, 4)),
            dma((CHUNKS, 2)),
            dma((CHUNKS, 2)),
            dma((CHUNKS, len(SPANS), 4)),
            dma((CHUNKS, len(SPANS), 4)),
            dma((2 * PIECES,)),
            dma((2 * PIECES,)),
        ],
        compiler_params=pltpu.CompilerParams(collective_id=0, has_side_effects=True),
        name="correlate",
    )(tables, inverses, own)
    half = half.astype(f32)
    return jnp.where(lax.axis_index("win") == 0, half, -half) + theirs.astype(f32)


def solution(mesh):
    rows = mesh.shape["cable"] // ROW
    return jax.shard_map(
        functools.partial(body, rows),
        mesh=mesh,
        in_specs=(P(None, "cable", "win"),),
        out_specs=P("cable", None, "win"),
        check_vma=False,
    )
```
